32 devices in a mesh: gx: 8 (over z, y), gy: 4 (over x, core).
Axes of the slice: x: 2, y: 2, z: 4, core: 2. Of those that a mesh axis runs over, the one named last changes fastest.
Arguments:
- ice_rhs: float32 [2, 512, 1024], P(None, 'gx', 'gy'), may hold values from -18.6 to 18.6
- ice_guess: float32 [2, 512, 1024], P(None, 'gx', 'gy'), may hold values from -9.3 to 9.3
- ocean_rhs: float32 [512, 1024], P('gx', 'gy'), may hold values from -18.6 to 18.6
- ocean_guess: float32 [512, 1024], P('gx', 'gy'), may hold values from -9.3 to 9.3
- ice_diag: float32 [512, 1024], P('gx', 'gy'), may hold values from 1 to 4
- ice_visc: float32 [512, 1024], P('gx', 'gy'), may hold values from 0.5 to 1.5
- coriolis: float32 [512, 1024], P('gx', 'gy'), may hold values from -1.5 to 1.5
- depth_factor: float32 [512, 1024], P('gx', 'gy'), may hold values from 1 to 3
- wet_mask: int32 [512, 1024], P('gx', 'gy'), may hold values 0 or 1
- ice_mask: int32 [512, 1024], P('gx', 'gy'), may hold values from 0 to 1, as said below
Outputs:
- ice_velocity: float32 [2, 512, 1024], P(None, 'gx', 'gy')
- ocean_level: float32 [512, 1024], P('gx', 'gy')
The draws below stay inside these ranges and needn't reach their ends.
Inputs may be any that keep to these rules, and one draw needn't show every extreme that they name: `ice_mask`: 1 where sea ice covers the cell.
All inputs are finite; a program needn't handle non-finite values. No bound on the sum of `wet_mask` on one device may be relied on, other than what follows from the above.
Results may differ from the reference program's by a relative error of at most 0.00005.
Values sent between devices are 32-bit elements; how exact they have to be, the bound alone decides.
A program may use at most 64 MiB of HBM per device.

```python
import math
import jax
import jax.numpy as jnp
from jax import lax

NX = 512
NY = 1024


def draw_ice_mask(key, part):
    rows = lax.broadcasted_iota(jnp.int32, (NX, NY), 1)
    polar = jnp.logical_or(rows * 8 >= 5 * NY, rows * 8 < 2 * NY)
    limit = jnp.where(polar, 85, 6)
    rolled = jax.random.randint(jax.random.fold_in(key, 17), (NX, NY), 0, 100)
    return (rolled < limit).astype(jnp.int32)


def northern_field(key, shape, scale):
    rows = lax.broadcasted_iota(jnp.int32, shape, len(shape) - 1).astype(jnp.float32)
    envelope = 0.1 + 3.0 * jnp.exp(-(NY - 1 - rows) / 32.0)
    noise = jnp.clip(jax.random.normal(key, shape, jnp.float32), -6.0, 6.0)
    return (scale * noise * envelope).astype(jnp.float32)


def draw_ice_rhs(key, part):
    return northern_field(jax.random.fold_in(key, 101), (2, NX, NY), 1.0)


def draw_ice_guess(key, part):
    return northern_field(jax.random.fold_in(key, 202), (2, NX, NY), 0.5)


def draw_ocean_rhs(key, part):
    return northern_field(jax.random.fold_in(key, 303), (NX, NY), 1.0)


def draw_ocean_guess(key, part):
    return northern_field(jax.random.fold_in(key, 404), (NX, NY), 0.5)


def plant(values, rng, smallest, high):
    longest = values.shape.index(max(values.shape))
    spots = []
    for shift in (0, 1):
        where = [jax.random.randint(jax.random.fold_in(rng, axis), (), 0, length) for axis, length in enumerate(values.shape)]
        where[longest] = (where[longest] + shift) % values.shape[longest]
        spots.append(tuple(where))
    return values.at[spots[0]].set(smallest).at[spots[1]].set(high)


def shard_levels(stream_key, dims, shards, low, high):
    def one(position, blocks):
        draws = jax.random.uniform(jax.random.fold_in(jax.random.fold_in(stream_key, 6), position), (blocks,), jnp.float32, low / len(shards), high / len(shards))
        return jnp.repeat(jnp.exp(draws), dims[position] // blocks).reshape((-1,) + (1,) * (len(dims) - position - 1))

    level = one(*shards[0])
    for cut in shards[1:]:
        level = level * one(*cut)
    return level


def setup_inputs(seed: int = 0) -> dict:
    streams_of = jax.random.split(jax.random.key(seed), 11)
    return {
        "ice_rhs": draw_ice_rhs(jax.random.fold_in(streams_of[10], 71), 0),
        "ice_guess": draw_ice_guess(jax.random.fold_in(streams_of[10], 71), 0),
        "ocean_rhs": draw_ocean_rhs(jax.random.fold_in(streams_of[10], 71), 0),
        "ocean_guess": draw_ocean_guess(jax.random.fold_in(streams_of[10], 71), 0),
        "ice_diag": jnp.clip(jnp.exp(math.log(4.0) - 1.3862944 * jax.random.uniform(streams_of[4], (NX, NY), jnp.float32) ** shard_levels(streams_of[4], (NX, NY), ((0, 8), (1, 4)), -0.2, 0.2)), 1.0, 4.0),
        "ice_visc": jnp.clip(jnp.exp(math.log(1.5) - 1.0986123 * jax.random.uniform(streams_of[5], (NX, NY), jnp.float32) ** shard_levels(streams_of[5], (NX, NY), ((0, 8), (1, 4)), -0.2, 0.2)), 0.5, 1.5),
        "coriolis": jnp.clip(jax.random.uniform(streams_of[6], (NX, NY), jnp.float32, -1.5, 1.5) * shard_levels(streams_of[6], (NX, NY), ((0, 8), (1, 4)), -0.4, 0.0), -1.5, 1.5),
        "depth_factor": jnp.clip(jnp.exp(math.log(3.0) - 1.0986123 * jax.random.uniform(streams_of[7], (NX, NY), jnp.float32) ** shard_levels(streams_of[7], (NX, NY), ((0, 8), (1, 4)), -0.2, 0.2)), 1.0, 3.0),
        "wet_mask": plant((jax.random.randint(streams_of[8], (NX, NY), 0, 5) < 4).astype(jnp.int32), jax.random.fold_in(streams_of[8], 1), 0, 1),
        "ice_mask": draw_ice_mask(jax.random.fold_in(streams_of[10], 71), 0),
    }


def neighbours(q):
    signs = jnp.array([-1.0, -1.0, 1.0], jnp.float32)[:, None]
    east = jnp.roll(q, -1, axis=1)
    west = jnp.roll(q, 1, axis=1)
    ghost = signs * q[:, ::-1, -1]
    north = jnp.concatenate([q[:, :, 1:], ghost[:, :, None]], axis=2)
    south = jnp.concatenate([jnp.zeros_like(q[:, :, :1]), q[:, :, :-1]], axis=2)
    return east + west + north + south

def operate(field, act, root, diag, coriolis):
    q = act * root * field
    lap = 4.0 * q - neighbours(q)
    turn = jnp.stack([-coriolis * field[1], coriolis * field[0], jnp.zeros_like(coriolis)])
    return act * (diag * field + root * lap + turn) + (1.0 - act) * field

def reference(ice_rhs, ice_guess, ocean_rhs, ocean_guess, ice_diag, ice_visc, coriolis, depth_factor, wet_mask, ice_mask):
    wet = wet_mask.astype(jnp.float32)
    active = wet * ice_mask.astype(jnp.float32)
    act = jnp.stack([active, active, wet])
    root = jnp.stack([ice_visc, ice_visc, depth_factor])
    diag = jnp.stack([ice_diag, ice_diag, jnp.ones_like(ice_diag)])
    inverse = 1.0 / (act * (diag + 4.0 * root * root) + 1.0 - act)

    def apply(ice_part, ocean_part):
        out = operate(jnp.concatenate([ice_part, ocean_part[None]]), act, root, diag, coriolis)
        return (out[:2], out[2])
    ice_start, ocean_start = apply(ice_guess, ocean_guess)
    r = ice_rhs - ice_start
    ro = ocean_rhs - ocean_start
    beta = jnp.sqrt(jnp.sum(r * r))
    v1 = r / beta
    z1 = inverse[:2] * v1
    z0 = inverse[2] * ro
    w1, ap0 = apply(z1, z0)
    h11 = jnp.sum(w1 * v1)
    other = w1 - h11 * v1
    h21 = jnp.sqrt(jnp.sum(other * other))
    v2 = other / h21
    z2 = inverse[:2] * v2
    rz0 = jnp.sum(ro * z0)
    alpha0 = rz0 / jnp.sum(z0 * ap0)
    level = ocean_guess + alpha0 * z0
    ro1 = ro - alpha0 * ap0
    zn = inverse[2] * ro1
    rz1 = jnp.sum(ro1 * zn)
    p1 = zn + rz1 / rz0 * z0
    w2, ap1 = apply(z2, p1)
    alpha1 = rz1 / jnp.sum(p1 * ap1)
    level = level + alpha1 * p1
    h12 = jnp.sum(w2 * v1)
    h22 = jnp.sum(w2 * v2)
    rest = w2 - h12 * v1 - h22 * v2
    h32sq = jnp.sum(rest * rest)
    g11 = h11 * h11 + h21 * h21
    g12 = h11 * h12 + h21 * h22
    g22 = h12 * h12 + h22 * h22 + h32sq
    first_rhs = beta * h11
    second_rhs = beta * h12
    det = g11 * g22 - g12 * g12
    y_first = (g22 * first_rhs - g12 * second_rhs) / det
    y_second = (g11 * second_rhs - g12 * first_rhs) / det
    velocity = ice_guess + y_first * z1 + y_second * z2
    return (velocity, level)
```

```python
import functools

import jax
import jax.numpy as jnp
from jax import lax
from jax.experimental import pallas as pl
from jax.experimental.pallas import tpu as pltpu
from jax.sharding import PartitionSpec as P

MESH = pl.DeviceIdType.MESH
LANES = 128
ROWS = 32
WIDTHS = (3, 3, 3, 2, 2, 2, 2, 2, 2, 2, 2)
PLACES = tuple(sum(WIDTHS[:i]) for i in range(len(WIDTHS)))
EAST, WEST, NORTH, SOUTH, NE, NW, SE, SW = range(8)
FLAT_LIMIT = 64
SUMS = 9


def flipped_rows(x):
    tiles = [x[k : k + 8] for k in range(0, x.shape[0], 8)][::-1]
    x = jnp.concatenate(tiles, axis=0)
    place = lax.broadcasted_iota(jnp.int32, x.shape, 0)
    size = x.shape[0]
    for bit in (1, 2, 4):
        x = jnp.where((place & bit) == 0, pltpu.roll(x, size - bit, 0), pltpu.roll(x, bit, 0))
    return x


def flipped_lanes(x):
    place = lax.broadcasted_iota(jnp.int32, x.shape, 1)
    for bit in (1, 2, 4, 8, 16, 32, 64):
        x = jnp.where((place & bit) == 0, pltpu.roll(x, LANES - bit, 1), pltpu.roll(x, bit, 1))
    return x


def rolled(x, by, axis):
    return pltpu.roll(x, by % x.shape[axis], axis)


def beside(x):
    return (rolled(x, 1, 0) + rolled(x, -1, 0)) + (rolled(x, 1, 1) + rolled(x, -1, 1))


def two_by_two(g11, g12, g22, f1, f2):
    det = g11 * g22 - g12 * g12
    good = det > 0.0
    safe = jnp.where(good, det, 1.0)
    first = jnp.where(good, (g22 * f1 - g12 * f2) / safe, f1 / g11)
    second = jnp.where(good, (g11 * f2 - g12 * f1) / safe, 0.0)
    return first, second


def kernel(sizes, *refs):
    gx, gy, rows, cols = sizes
    total = gx * gy
    ins = refs[:10]
    out_ice, out_ocean = refs[10:12]
    held = refs[12:22]
    (
        ext, inv_ref, send_e, send_w, send_n, send_s, send_ne, send_nw,
        recv_e, recv_w, recv_n, recv_s, recv_corner, wide_e, wide_w, sums,
        in_sem, send_sem, recv_sem, sum_send, sum_recv,
    ) = refs[22:]
    x = lax.axis_index("gx")
    y = lax.axis_index("gy")
    me = x * gy + y
    top = y == gy - 1
    bottom = y == 0

    loads = [pltpu.make_async_copy(ins[k], held[k], in_sem.at[k]) for k in range(10)]
    for load in loads:
        load.start()

    flat = total <= FLAT_LIMIT
    barrier = pltpu.get_barrier_semaphore()

    def greet(px, py):
        pl.semaphore_signal(barrier, inc=1, device_id=(px, py), device_id_type=MESH)

    east, west = lax.rem(x + 1, gx), lax.rem(x + gx - 1, gx)
    if flat:
        @pl.loop(1, total)
        def _(k):
            other = lax.rem(me + k, total)
            greet(other // gy, lax.rem(other, gy))
    else:
        @pl.loop(1, gx)
        def _(k):
            greet(lax.rem(x + k, gx), y)

        @pl.loop(1, gy)
        def _(k):
            greet(x, lax.rem(y + k, gy))

        @pl.when(jnp.logical_not(top))
        def _():
            greet(east, y + 1)
            greet(west, y + 1)

        @pl.when(jnp.logical_not(bottom))
        def _():
            greet(east, y - 1)
            greet(west, y - 1)

    @pl.when(bottom)
    def _():
        recv_s[...] = jnp.zeros_like(recv_s)
        recv_corner[SE - NE] = jnp.zeros((ROWS, LANES), jnp.float32)
        recv_corner[SW - NE] = jnp.zeros((ROWS, LANES), jnp.float32)

    for load in loads:
        load.wait()
    rhs, guess, orhs, oguess, mass, visc, cor, depth, wetm, icem = held
    wet = wetm[...].astype(jnp.float32)
    active = wet * icem[...].astype(jnp.float32)
    visc = visc[...]
    depth = depth[...]
    mass = mass[...]
    cor = cor[...]
    gu, gv, gs = guess[0], guess[1], oguess[...]
    ai = active * visc
    ao = wet * depth
    full_i = active * (mass + 4.0 * visc * visc) + 1.0 - active
    full_o = wet * (1.0 + 4.0 * depth * depth) + 1.0 - wet
    pi = 1.0 / full_i
    po = 1.0 / full_o
    inv_ref[0] = pi
    inv_ref[1] = po
    ac = active * cor
    fields = [
        ai * gu,
        ai * gv,
        ao * gs,
        rhs[0] - (full_i * gu - ac * gv),
        rhs[1] - (full_i * gv + ac * gu),
        orhs[...] - full_o * gs,
        ai,
        ao,
        ai * pi,
        ao * po,
        ac * pi,
    ]
    for k, field in enumerate(fields):
        ext[k, 0:rows, 0:cols] = field

    send_e[...] = jnp.zeros_like(send_e)
    send_w[...] = jnp.zeros_like(send_w)
    for k, (width, place) in enumerate(zip(WIDTHS, PLACES)):
        send_w[place : place + width, :] = ext[k, 0:width, 0:cols]
        start = ROWS - place - width
        send_e[start : start + width, :] = ext[k, rows - width : rows, 0:cols]
    lane = lax.broadcasted_iota(jnp.int32, (rows, LANES), 1)
    low = jnp.zeros((rows, LANES), jnp.float32)
    high = jnp.zeros((rows, LANES), jnp.float32)
    for k, (width, place) in enumerate(zip(WIDTHS, PLACES)):
        first = ext[k, 0:rows, 0:LANES]
        last = ext[k, 0:rows, cols - LANES : cols]
        low = jnp.where((lane >= place) & (lane < place + width), rolled(first, place, 1), low)
        start = LANES - place - width
        high = jnp.where((lane >= start) & (lane < start + width), rolled(last, -place, 1), high)
    send_s[...] = low

    @pl.when(jnp.logical_not(top))
    def _():
        send_n[...] = high
        send_ne[...] = send_e[:, cols - LANES : cols]
        send_nw[...] = send_w[:, cols - LANES : cols]

    def negated(place):
        return (place < 6) | ((place >= 9) & (place < 13))

    @pl.when(top)
    def _():
        sign = jnp.where(negated(lane), -1.0, 1.0)
        send_n[...] = sign * flipped_lanes(flipped_rows(high))
        row = lax.broadcasted_iota(jnp.int32, (ROWS, LANES), 0)
        e_side = flipped_lanes(flipped_rows(send_e[:, cols - LANES : cols]))
        send_ne[...] = jnp.where(negated(row), -e_side, e_side)
        w_side = flipped_lanes(flipped_rows(send_w[:, cols - LANES : cols]))
        send_nw[...] = jnp.where(negated(ROWS - 1 - row), -w_side, w_side)

    if flat:
        pl.semaphore_wait(barrier, total - 1)
    else:
        diagonals = 2 * (jnp.where(top, 0, 1) + jnp.where(bottom, 0, 1))
        pl.semaphore_wait(barrier, gx - 1 + gy - 1 + diagonals)

    def copy(source, where, slot, px, py):
        return pltpu.make_async_remote_copy(
            src_ref=source,
            dst_ref=where,
            send_sem=send_sem.at[slot],
            recv_sem=recv_sem.at[slot],
            device_id=(px, py),
            device_id_type=MESH,
        )

    mirror = gx - 1 - x
    fold_e = lax.rem(mirror + gx - 1, gx)
    fold_w = lax.rem(mirror + 1, gx)
    corner = [recv_corner.at[k] for k in range(4)]
    to_e = copy(send_e, recv_w, WEST, east, y)
    to_w = copy(send_w, recv_e, EAST, west, y)
    plain_n = [
        copy(send_n, recv_s, SOUTH, x, y + 1),
        copy(send_ne, corner[SW - NE], SW, east, y + 1),
        copy(send_nw, corner[SE - NE], SE, west, y + 1),
    ]
    fold_n = copy(send_n, recv_n, NORTH, mirror, y)
    fold_ne = copy(send_ne, corner[NE - NE], NE, fold_e, y)
    fold_nw = copy(send_nw, corner[NW - NE], NW, fold_w, y)
    plain_s = [
        copy(send_s, recv_n, NORTH, x, y - 1),
        copy(send_e.at[:, 0:LANES], corner[NW - NE], NW, east, y - 1),
        copy(send_w.at[:, 0:LANES], corner[NE - NE], NE, west, y - 1),
    ]
    away_e = top & (fold_e != x)
    away_w = top & (fold_w != x)

    to_e.start()
    to_w.start()

    @pl.when(top)
    def _():
        fold_n.start()

    @pl.when(away_e)
    def _():
        fold_ne.start()

    @pl.when(away_w)
    def _():
        fold_nw.start()

    @pl.when(top & (fold_e == x))
    def _():
        recv_corner[NE - NE] = send_ne[...]

    @pl.when(top & (fold_w == x))
    def _():
        recv_corner[NW - NE] = send_nw[...]

    @pl.when(jnp.logical_not(top))
    def _():
        for c in plain_n:
            c.start()

    @pl.when(jnp.logical_not(bottom))
    def _():
        for c in plain_s:
            c.start()

    @pl.when(jnp.logical_not(bottom))
    def _():
        for c in plain_n:
            c.wait_recv()

    plain_s[0].wait_recv()

    @pl.when(jnp.logical_not(top & (fold_e == x)))
    def _():
        plain_s[2].wait_recv()

    @pl.when(jnp.logical_not(top & (fold_w == x)))
    def _():
        plain_s[1].wait_recv()

    to_e.wait_recv()
    to_w.wait_recv()

    from_n = recv_n[...]
    from_s = recv_s[...]
    wide_e[:, 0:cols] = recv_e[...]
    wide_w[:, 0:cols] = recv_w[...]
    side = lax.broadcasted_iota(jnp.int32, (ROWS, LANES), 1) < LANES // 2
    wide_e[:, cols : cols + LANES] = jnp.where(side, recv_corner[NE - NE], recv_corner[SE - NE])
    wide_w[:, cols : cols + LANES] = jnp.where(side, recv_corner[NW - NE], recv_corner[SW - NE])
    upper = lax.broadcasted_iota(jnp.int32, (8, cols + LANES), 0) < 4
    for k, place in enumerate(PLACES):
        ext[k, 0:rows, cols : cols + LANES] = jnp.where(
            lane < LANES // 2, rolled(from_n, -place, 1), rolled(from_s, place, 1)
        )
        end = ROWS - place
        ext[k, rows : rows + 8, :] = jnp.where(
            upper, wide_e[place : place + 8, :], wide_w[end - 8 : end, :]
        )

    ai, ao, si, so, c = (ext[k] for k in range(6, 11))
    ru = ext[3] + ai * beside(ext[0])
    rv = ext[4] + ai * beside(ext[1])
    rs = ext[5] + ao * beside(ext[2])
    nu = ai * beside(si * ru) + c * rv
    nv = ai * beside(si * rv) - c * ru
    ns = ao * beside(so * rs)
    mu = ai * beside(si * nu) + c * nv
    mv = ai * beside(si * nv) - c * nu
    ms = ao * beside(so * ns)

    def own(value):
        return value[0:rows, 0:cols]

    ru, rv, rs, nu, nv, ns, mu, mv, ms = map(own, (ru, rv, rs, nu, nv, ns, mu, mv, ms))
    pi, po = inv_ref[0], inv_ref[1]
    e1u, e1v, e1s = ru - nu, rv - nv, rs - ns
    e2u, e2v, e2s = nu - mu, nv - mv, ns - ms
    prs, pns = po * rs, po * ns
    products = [
        e1u * e1u + e1v * e1v,
        e1u * e2u + e1v * e2v,
        e2u * e2u + e2v * e2v,
        e1u * ru + e1v * rv,
        e2u * ru + e2v * rv,
        prs * e1s,
        pns * e1s,
        pns * e2s,
        pns * rs,
    ]
    spot = lax.broadcasted_iota(jnp.int32, (1, LANES), 1)
    packed = jnp.zeros((1, LANES), jnp.float32)
    for k, product in enumerate(products):
        packed = jnp.where(spot == k, jnp.sum(product, keepdims=True), packed)

    def exchange(slot, count, mine, device, number):
        slot[mine] = packed_now[0]

        def one(k):
            return pltpu.make_async_remote_copy(
                src_ref=slot.at[mine],
                dst_ref=slot.at[mine],
                send_sem=sum_send.at[number],
                recv_sem=sum_recv.at[number],
                device_id=device(k),
                device_id_type=MESH,
            )

        @pl.loop(1, count)
        def _(k):
            one(k).start()

        most = slot.at[pl.ds(0, count - 1)]
        pltpu.make_async_copy(most, most, sum_recv.at[number]).wait()
        result = jnp.sum(slot[...], axis=0)
        pltpu.make_async_copy(most, most, sum_send.at[number]).wait()
        return result

    packed_now = [packed]
    if flat:
        def anyone(k):
            other = lax.rem(me + k, total)
            return (other // gy, lax.rem(other, gy))

        packed = exchange(sums, total, me, anyone, 0)
    else:
        packed_now[0] = exchange(
            sums.at[pl.ds(0, gx)], gx, x, lambda k: (lax.rem(x + k, gx), y), 0
        )
        packed = exchange(
            sums.at[pl.ds(gx, gy)], gy, y, lambda k: (x, lax.rem(y + k, gy)), 1
        )
    s = [
        jnp.sum(jnp.where(spot == k, packed, 0.0), axis=1, keepdims=True) for k in range(SUMS)
    ]
    y1, y2 = two_by_two(s[0], s[1], s[2], s[3], s[4])
    d1, d2 = two_by_two(s[5], s[6], s[7], s[5] + s[8], s[8])
    out_ice[0] = held[1][0] + pi * (y1 * ru + y2 * nu)
    out_ice[1] = held[1][1] + pi * (y1 * rv + y2 * nv)
    out_ocean[...] = held[3][...] + d1 * prs + d2 * pns

    to_e.wait_send()
    to_w.wait_send()

    @pl.when(top)
    def _():
        fold_n.wait_send()

    @pl.when(away_e)
    def _():
        fold_ne.wait_send()

    @pl.when(away_w)
    def _():
        fold_nw.wait_send()

    @pl.when(jnp.logical_not(top))
    def _():
        for c in plain_n:
            c.wait_send()

    @pl.when(jnp.logical_not(bottom))
    def _():
        for c in plain_s:
            c.wait_send()


def solution(mesh):
    gx, gy = mesh.shape["gx"], mesh.shape["gy"]

    def body(*args):
        _, rows, cols = args[0].shape
        slots = gx * gy if gx * gy <= FLAT_LIMIT else gx + gy
        f32 = jnp.float32
        edge = pltpu.VMEM((rows, LANES), f32)
        strip = pltpu.VMEM((ROWS, cols), f32)
        corner = pltpu.VMEM((ROWS, LANES), f32)
        wide = pltpu.VMEM((ROWS, cols + LANES), f32)
        return pl.pallas_call(
            functools.partial(kernel, (gx, gy, rows, cols)),
            out_shape=(
                jax.ShapeDtypeStruct((2, rows, cols), f32),
                jax.ShapeDtypeStruct((rows, cols), f32),
            ),
            in_specs=[pl.BlockSpec(memory_space=pl.ANY)] * 10,
            out_specs=(pl.BlockSpec(memory_space=pltpu.VMEM),) * 2,
            scratch_shapes=[pltpu.VMEM(a.shape, a.dtype) for a in args]
            + [
                pltpu.VMEM((len(WIDTHS), rows + 8, cols + LANES), f32),
                pltpu.VMEM((2, rows, cols), f32),
                strip, strip, edge, edge, corner, corner,
                strip, strip, edge, edge, pltpu.VMEM((4, ROWS, LANES), f32), wide, wide,
                pltpu.VMEM((slots, 1, LANES), f32),
                pltpu.SemaphoreType.DMA((10,)),
                pltpu.SemaphoreType.DMA((8,)),
                pltpu.SemaphoreType.DMA((8,)),
                pltpu.SemaphoreType.DMA((2,)),
                pltpu.SemaphoreType.DMA((2,)),
            ],
            compiler_params=pltpu.CompilerParams(collective_id=0, has_side_effects=True),
            name="picard",
        )(*args)

    grid3, grid2 = P(None, "gx", "gy"), P("gx", "gy")
    return jax.shard_map(
        body,
        mesh=mesh,
        in_specs=(grid3, grid3) + (grid2,) * 8,
        out_specs=(grid3, grid2),
        check_vma=False,
    )
```

```python
import functools

import jax
import jax.numpy as jnp
from jax import lax
from jax.experimental import pallas as pl
from jax.experimental.pallas import tpu as pltpu
from jax.sharding import PartitionSpec as P

MESH = pl.DeviceIdType.MESH
LANES = 128
ROWS = 24
WIDTHS = (3, 3, 3, 2, 2, 2, 2, 2, 2, 2, 1)
PLACES = tuple(sum(WIDTHS[:i]) for i in range(len(WIDTHS)))
EAST, WEST, NORTH, SOUTH, NE, NW, SE, SW = range(8)
FLAT_LIMIT = 64
SUMS = 9


def flipped_rows(x):
    tiles = [x[k : k + 8] for k in range(0, x.shape[0], 8)][::-1]
    x = jnp.concatenate(tiles, axis=0)
    place = lax.broadcasted_iota(jnp.int32, x.shape, 0)
    size = x.shape[0]
    for bit in (1, 2, 4):
        x = jnp.where((place & bit) == 0, pltpu.roll(x, size - bit, 0), pltpu.roll(x, bit, 0))
    return x


def flipped_lanes(x):
    place = lax.broadcasted_iota(jnp.int32, x.shape, 1)
    for bit in (1, 2, 4, 8, 16, 32, 64):
        x = jnp.where((place & bit) == 0, pltpu.roll(x, LANES - bit, 1), pltpu.roll(x, bit, 1))
    return x


def rolled(x, by, axis):
    return pltpu.roll(x, by % x.shape[axis], axis)


def beside(x):
    return (rolled(x, 1, 0) + rolled(x, -1, 0)) + (rolled(x, 1, 1) + rolled(x, -1, 1))


def two_by_two(g11, g12, g22, f1, f2):
    det = g11 * g22 - g12 * g12
    good = det > 0.0
    safe = jnp.where(good, det, 1.0)
    first = jnp.where(good, (g22 * f1 - g12 * f2) / safe, f1 / g11)
    second = jnp.where(good, (g11 * f2 - g12 * f1) / safe, 0.0)
    return first, second


def kernel(sizes, *refs):
    gx, gy, rows, cols = sizes
    total = gx * gy
    ins = refs[:10]
    out_ice, out_ocean = refs[10:12]
    held = refs[12:22]
    (
        ext, inv_ref, send_e, send_w, send_n, send_s,
        recv_e, recv_w, recv_n, recv_s, recv_corner, scaled, sums,
        in_sem, send_sem, recv_sem, sum_send, sum_recv,
    ) = refs[22:]
    x = lax.axis_index("gx")
    y = lax.axis_index("gy")
    me = x * gy + y
    top = y == gy - 1
    bottom = y == 0

    loads = [pltpu.make_async_copy(ins[k], held[k], in_sem.at[k]) for k in range(10)]
    for load in loads:
        load.start()

    flat = total <= FLAT_LIMIT
    barrier = pltpu.get_barrier_semaphore()

    def greet(px, py):
        pl.semaphore_signal(barrier, inc=1, device_id=(px, py), device_id_type=MESH)

    east, west = lax.rem(x + 1, gx), lax.rem(x + gx - 1, gx)
    if flat:
        @pl.loop(1, total)
        def _(k):
            other = lax.rem(me + k, total)
            greet(other // gy, lax.rem(other, gy))
    else:
        @pl.loop(1, gx)
        def _(k):
            greet(lax.rem(x + k, gx), y)

        @pl.loop(1, gy)
        def _(k):
            greet(x, lax.rem(y + k, gy))

        @pl.when(jnp.logical_not(top))
        def _():
            greet(east, y + 1)
            greet(west, y + 1)

        @pl.when(jnp.logical_not(bottom))
        def _():
            greet(east, y - 1)
            greet(west, y - 1)

    @pl.when(bottom)
    def _():
        recv_s[...] = jnp.zeros_like(recv_s)
        recv_corner[SE - NE] = jnp.zeros((8, LANES), jnp.float32)
        recv_corner[SW - NE] = jnp.zeros((8, LANES), jnp.float32)

    for load in loads:
        load.wait()
    rhs, guess, orhs, oguess, mass, visc, cor, depth, wetm, icem = held
    wet = wetm[...].astype(jnp.float32)
    active = wet * icem[...].astype(jnp.float32)
    visc = visc[...]
    depth = depth[...]
    mass = mass[...]
    cor = cor[...]
    gu, gv, gs = guess[0], guess[1], oguess[...]
    ai = active * visc
    ao = wet * depth
    full_i = active * (mass + 4.0 * visc * visc) + 1.0 - active
    full_o = wet * (1.0 + 4.0 * depth * depth) + 1.0 - wet
    pi = 1.0 / full_i
    po = 1.0 / full_o
    inv_ref[0] = pi
    inv_ref[1] = po
    ac = active * cor
    fields = [
        ai * gu,
        ai * gv,
        ao * gs,
        rhs[0] - (full_i * gu - ac * gv),
        rhs[1] - (full_i * gv + ac * gu),
        orhs[...] - full_o * gs,
        ai,
        ao,
        ai * pi,
        ao * po,
        ac * pi,
    ]
    for k, field in enumerate(fields):
        ext[k, 0:rows, 0:cols] = field

    send_e[...] = jnp.zeros_like(send_e)
    send_w[...] = jnp.zeros_like(send_w)
    for k, (width, place) in enumerate(zip(WIDTHS, PLACES)):
        send_w[place : place + width, :] = ext[k, 0:width, 0:cols]
        start = ROWS - place - width
        send_e[start : start + width, :] = ext[k, rows - width : rows, 0:cols]
    lane = lax.broadcasted_iota(jnp.int32, (rows, LANES), 1)
    low = jnp.zeros((rows, LANES), jnp.float32)
    high = jnp.zeros((rows, LANES), jnp.float32)
    for k, (width, place) in enumerate(zip(WIDTHS, PLACES)):
        first = ext[k, 0:rows, 0:LANES]
        last = ext[k, 0:rows, cols - LANES : cols]
        low = jnp.where((lane >= place) & (lane < place + width), rolled(first, place, 1), low)
        start = LANES - place - width
        high = jnp.where((lane >= start) & (lane < start + width), rolled(last, -place, 1), high)
    send_s[...] = low

    @pl.when(jnp.logical_not(top))
    def _():
        send_n[...] = high

    def negated(place):
        return (place < 6) | ((place >= 9) & (place < 13))

    @pl.when(top)
    def _():
        sign = jnp.where(negated(lane), -1.0, 1.0)
        send_n[...] = sign * flipped_lanes(flipped_rows(high))

    if flat:
        pl.semaphore_wait(barrier, total - 1)
    else:
        diagonals = 2 * (jnp.where(top, 0, 1) + jnp.where(bottom, 0, 1))
        pl.semaphore_wait(barrier, gx - 1 + gy - 1 + diagonals)

    def copy(source, where, slot, px, py):
        return pltpu.make_async_remote_copy(
            src_ref=source,
            dst_ref=where,
            send_sem=send_sem.at[slot],
            recv_sem=recv_sem.at[slot],
            device_id=(px, py),
            device_id_type=MESH,
        )

    mirror = gx - 1 - x
    fold_e = lax.rem(mirror + gx - 1, gx)
    fold_w = lax.rem(mirror + 1, gx)
    corner = [recv_corner.at[k] for k in range(4)]
    to_e = copy(send_e, recv_w.at[pl.ds(8, ROWS)], WEST, east, y)
    to_w = copy(send_w, recv_e.at[pl.ds(0, ROWS)], EAST, west, y)
    n_first, n_last = send_n.at[pl.ds(0, 8)], send_n.at[pl.ds(rows - 8, 8)]
    s_first, s_last = send_s.at[pl.ds(0, 8)], send_s.at[pl.ds(rows - 8, 8)]
    plain_n = [
        copy(send_n, recv_s, SOUTH, x, y + 1),
        copy(n_last, corner[SW - NE], SW, east, y + 1),
        copy(n_first, corner[SE - NE], SE, west, y + 1),
    ]
    fold_n = copy(send_n, recv_n, NORTH, mirror, y)
    fold_ne = copy(n_first, corner[NE - NE], NE, fold_e, y)
    fold_nw = copy(n_last, corner[NW - NE], NW, fold_w, y)
    plain_s = [
        copy(send_s, recv_n, NORTH, x, y - 1),
        copy(s_last, corner[NW - NE], NW, east, y - 1),
        copy(s_first, corner[NE - NE], NE, west, y - 1),
    ]
    away_e = top & (fold_e != x)
    away_w = top & (fold_w != x)

    to_e.start()
    to_w.start()

    @pl.when(top)
    def _():
        fold_n.start()

    @pl.when(away_e)
    def _():
        fold_ne.start()

    @pl.when(away_w)
    def _():
        fold_nw.start()

    @pl.when(top & (fold_e == x))
    def _():
        recv_corner[NE - NE] = send_n[0:8]

    @pl.when(top & (fold_w == x))
    def _():
        recv_corner[NW - NE] = send_n[rows - 8 : rows]

    @pl.when(jnp.logical_not(top))
    def _():
        for c in plain_n:
            c.start()

    @pl.when(jnp.logical_not(bottom))
    def _():
        for c in plain_s:
            c.start()

    @pl.when(jnp.logical_not(bottom))
    def _():
        for c in plain_n:
            c.wait_recv()

    plain_s[0].wait_recv()

    @pl.when(jnp.logical_not(top & (fold_e == x)))
    def _():
        plain_s[2].wait_recv()

    @pl.when(jnp.logical_not(top & (fold_w == x)))
    def _():
        plain_s[1].wait_recv()

    to_e.wait_recv()
    to_w.wait_recv()

    half = lax.broadcasted_iota(jnp.int32, (8, LANES), 0) < 4
    corner_n = jnp.where(half, recv_corner[NE - NE], recv_corner[NW - NE])
    corner_s = jnp.where(half, recv_corner[SE - NE], recv_corner[SW - NE])
    from_n = jnp.concatenate([recv_n[...], corner_n], axis=0)
    from_s = jnp.concatenate([recv_s[...], corner_s], axis=0)
    near = lax.broadcasted_iota(jnp.int32, (rows + 8, LANES), 1) < LANES // 2
    upper = lax.broadcasted_iota(jnp.int32, (8, cols), 0) < 4
    for k, place in enumerate(PLACES):
        ext[k, :, cols : cols + LANES] = jnp.where(
            near, rolled(from_n, -place, 1), rolled(from_s, place, 1)
        )
        end = 8 + ROWS - place
        ext[k, rows : rows + 8, 0:cols] = jnp.where(
            upper, recv_e[place : place + 8, :], recv_w[end - 8 : end, :]
        )

    ai, ao, si, so, c = (ext[k] for k in range(6, 11))
    ru = ext[3] + ai * beside(ext[0])
    rv = ext[4] + ai * beside(ext[1])
    rs = ext[5] + ao * beside(ext[2])
    nu = ai * beside(si * ru) + c * rv
    nv = ai * beside(si * rv) - c * ru
    ns = ao * beside(so * rs)
    mu = ai * beside(si * nu) + c * nv
    mv = ai * beside(si * nv) - c * nu
    ms = ao * beside(so * ns)

    def own(value):
        return value[0:rows, 0:cols]

    ru, rv, rs, nu, nv, ns, mu, mv, ms = map(own, (ru, rv, rs, nu, nv, ns, mu, mv, ms))
    pi, po = inv_ref[0], inv_ref[1]
    e1u, e1v, e1s = ru - nu, rv - nv, rs - ns
    e2u, e2v, e2s = nu - mu, nv - mv, ns - ms
    prs, pns = po * rs, po * ns
    products = [
        e1u * e1u + e1v * e1v,
        e1u * e2u + e1v * e2v,
        e2u * e2u + e2v * e2v,
        e1u * ru + e1v * rv,
        e2u * ru + e2v * rv,
        prs * e1s,
        pns * e1s,
        pns * e2s,
        pns * rs,
    ]
    spot = lax.broadcasted_iota(jnp.int32, (1, LANES), 1)
    packed = jnp.zeros((1, LANES), jnp.float32)
    for k, product in enumerate(products):
        packed = jnp.where(spot == k, jnp.sum(product, keepdims=True), packed)

    def exchange(slot, count, mine, device, number, work=None):
        slot[mine] = packed_now[0]

        def one(k):
            return pltpu.make_async_remote_copy(
                src_ref=slot.at[mine],
                dst_ref=slot.at[mine],
                send_sem=sum_send.at[number],
                recv_sem=sum_recv.at[number],
                device_id=device(k),
                device_id_type=MESH,
            )

        @pl.loop(1, count)
        def _(k):
            one(k).start()

        if work is not None:
            work()
        most = slot.at[pl.ds(0, count - 1)]
        pltpu.make_async_copy(most, most, sum_recv.at[number]).wait()
        return jnp.sum(slot[...], axis=0)

    def scale():
        for k, value in enumerate((pi * ru, pi * rv, prs, pi * nu, pi * nv, pns)):
            scaled[k] = value

    packed_now = [packed]
    if flat:
        def anyone(k):
            other = lax.rem(me + k, total)
            return (other // gy, lax.rem(other, gy))

        packed = exchange(sums, total, me, anyone, 0, scale)
    else:
        packed_now[0] = exchange(
            sums.at[pl.ds(0, gx)], gx, x, lambda k: (lax.rem(x + k, gx), y), 0, scale
        )
        packed = exchange(
            sums.at[pl.ds(gx, gy)], gy, y, lambda k: (x, lax.rem(y + k, gy)), 1
        )
    s = [
        jnp.sum(jnp.where(spot == k, packed, 0.0), axis=1, keepdims=True) for k in range(SUMS)
    ]
    y1, y2 = two_by_two(s[0], s[1], s[2], s[3], s[4])
    d1, d2 = two_by_two(s[5], s[6], s[7], s[5] + s[8], s[8])
    out_ice[0] = held[1][0] + y1 * scaled[0] + y2 * scaled[3]
    out_ice[1] = held[1][1] + y1 * scaled[1] + y2 * scaled[4]
    out_ocean[...] = held[3][...] + d1 * scaled[2] + d2 * scaled[5]

    groups = [(sums, total)] if flat else [(sums.at[pl.ds(0, gx)], gx), (sums.at[pl.ds(gx, gy)], gy)]
    for number, (slot, count) in enumerate(groups):
        most = slot.at[pl.ds(0, count - 1)]
        pltpu.make_async_copy(most, most, sum_send.at[number]).wait()
    to_e.wait_send()
    to_w.wait_send()

    @pl.when(top)
    def _():
        fold_n.wait_send()

    @pl.when(away_e)
    def _():
        fold_ne.wait_send()

    @pl.when(away_w)
    def _():
        fold_nw.wait_send()

    @pl.when(jnp.logical_not(top))
    def _():
        for c in plain_n:
            c.wait_send()

    @pl.when(jnp.logical_not(bottom))
    def _():
        for c in plain_s:
            c.wait_send()


def store(ice, ocean, out_ice, out_ocean, sem):
    copies = [
        pltpu.make_async_copy(ice, out_ice, sem.at[0]),
        pltpu.make_async_copy(ocean, out_ocean, sem.at[1]),
    ]
    for c in copies:
        c.start()
    for c in copies:
        c.wait()


def solution(mesh):
    gx, gy = mesh.shape["gx"], mesh.shape["gy"]

    def body(*args):
        _, rows, cols = args[0].shape
        slots = gx * gy if gx * gy <= FLAT_LIMIT else gx + gy
        f32 = jnp.float32
        edge = pltpu.VMEM((rows, LANES), f32)
        strip = pltpu.VMEM((ROWS, cols), f32)
        tall = pltpu.VMEM((ROWS + 8, cols), f32)
        ice, ocean = pl.pallas_call(
            functools.partial(kernel, (gx, gy, rows, cols)),
            out_shape=(pltpu.VMEM((2, rows, cols), f32), pltpu.VMEM((rows, cols), f32)),
            in_specs=[pl.BlockSpec(memory_space=pl.ANY)] * 10,
            out_specs=(pl.BlockSpec(memory_space=pltpu.VMEM),) * 2,
            scratch_shapes=[pltpu.VMEM(a.shape, a.dtype) for a in args]
            + [
                pltpu.VMEM((len(WIDTHS), rows + 8, cols + LANES), f32),
                pltpu.VMEM((2, rows, cols), f32),
                strip, strip, edge, edge,
                tall, tall, edge, edge, pltpu.VMEM((4, 8, LANES), f32),
                pltpu.VMEM((6, rows, cols), f32),
                pltpu.VMEM((slots, 1, LANES), f32),
                pltpu.SemaphoreType.DMA((10,)),
                pltpu.SemaphoreType.DMA((8,)),
                pltpu.SemaphoreType.DMA((8,)),
                pltpu.SemaphoreType.DMA((2,)),
                pltpu.SemaphoreType.DMA((2,)),
            ],
            compiler_params=pltpu.CompilerParams(collective_id=0, has_side_effects=True),
            name="picard",
        )(*args)
        return pl.pallas_call(
            store,
            out_shape=(
                jax.ShapeDtypeStruct(ice.shape, f32),
                jax.ShapeDtypeStruct(ocean.shape, f32),
            ),
            in_specs=[pl.BlockSpec(memory_space=pltpu.VMEM)] * 2,
            out_specs=(pl.BlockSpec(memory_space=pl.ANY),) * 2,
            scratch_shapes=[pltpu.SemaphoreType.DMA((2,))],
            name="store",
        )(
            pltpu.with_memory_space_constraint(ice, pltpu.VMEM),
            pltpu.with_memory_space_constraint(ocean, pltpu.VMEM),
        )

    grid3, grid2 = P(None, "gx", "gy"), P("gx", "gy")
    return jax.shard_map(
        body,
        mesh=mesh,
        in_specs=(grid3, grid3) + (grid2,) * 8,
        out_specs=(grid3, grid2),
        check_vma=False,
    )
```

```python
import functools

import jax
import jax.numpy as jnp
from jax import lax
from jax.experimental import pallas as pl
from jax.experimental.pallas import tpu as pltpu
from jax.sharding import PartitionSpec as P

MESH = pl.DeviceIdType.MESH
LANES = 128
ROWS = 24
WIDTHS = (3, 3, 3, 2, 2, 2, 2, 2, 2, 2, 1)
PLACES = tuple(sum(WIDTHS[:i]) for i in range(len(WIDTHS)))
EAST, WEST, NORTH, SOUTH, NE, NW, SE, SW = range(8)
FLAT_LIMIT = 64
SUMS = 9


def flipped_rows(x):
    tiles = [x[k : k + 8] for k in range(0, x.shape[0], 8)][::-1]
    x = jnp.concatenate(tiles, axis=0)
    place = lax.broadcasted_iota(jnp.int32, x.shape, 0)
    size = x.shape[0]
    for bit in (1, 2, 4):
        x = jnp.where((place & bit) == 0, pltpu.roll(x, size - bit, 0), pltpu.roll(x, bit, 0))
    return x


def flipped_lanes(x):
    place = lax.broadcasted_iota(jnp.int32, x.shape, 1)
    for bit in (1, 2, 4, 8, 16, 32, 64):
        x = jnp.where((place & bit) == 0, pltpu.roll(x, LANES - bit, 1), pltpu.roll(x, bit, 1))
    return x


def rolled(x, by, axis):
    return pltpu.roll(x, by % x.shape[axis], axis)


def beside(x):
    return (rolled(x, 1, 0) + rolled(x, -1, 0)) + (rolled(x, 1, 1) + rolled(x, -1, 1))


def two_by_two(g11, g12, g22, f1, f2):
    det = g11 * g22 - g12 * g12
    good = det > 0.0
    safe = jnp.where(good, det, 1.0)
    first = jnp.where(good, (g22 * f1 - g12 * f2) / safe, f1 / g11)
    second = jnp.where(good, (g11 * f2 - g12 * f1) / safe, 0.0)
    return first, second


def kernel(sizes, *refs):
    gx, gy, rows, cols = sizes
    total = gx * gy
    ins = refs[:10]
    out_ice, out_ocean = refs[10:12]
    held = refs[12:22]
    (
        ext, inv_ref, send_e, send_w, send_n, send_s,
        recv_e, recv_w, recv_n, recv_s, recv_corner, scaled, sums,
        in_sem, send_sem, recv_sem, sum_send, sum_recv,
    ) = refs[22:]
    x = lax.axis_index("gx")
    y = lax.axis_index("gy")
    me = x * gy + y
    top = y == gy - 1
    bottom = y == 0

    loads = [pltpu.make_async_copy(ins[k], held[k], in_sem.at[k]) for k in range(10)]
    flat = total <= FLAT_LIMIT
    barrier = pltpu.get_barrier_semaphore()

    def greet(px, py):
        pl.semaphore_signal(barrier, inc=1, device_id=(px, py), device_id_type=MESH)

    east, west = lax.rem(x + 1, gx), lax.rem(x + gx - 1, gx)
    if flat:
        for step in range(gx):
            px = lax.rem(2 * gx - 1 - x + step, gx)
            for py in range(gy):

                @pl.when((px != x) | (py != y))
                def _():
                    greet(px, py)

    else:
        @pl.loop(1, gx)
        def _(k):
            greet(lax.rem(x + k, gx), y)

        @pl.loop(1, gy)
        def _(k):
            greet(x, lax.rem(y + k, gy))

        @pl.when(jnp.logical_not(top))
        def _():
            greet(east, y + 1)
            greet(west, y + 1)

        @pl.when(jnp.logical_not(bottom))
        def _():
            greet(east, y - 1)
            greet(west, y - 1)

    for load in loads:
        load.start()

    @pl.when(bottom)
    def _():
        recv_s[...] = jnp.zeros_like(recv_s)
        recv_corner[SE - NE] = jnp.zeros((8, LANES), jnp.float32)
        recv_corner[SW - NE] = jnp.zeros((8, LANES), jnp.float32)

    for load in loads:
        load.wait()
    rhs, guess, orhs, oguess, mass, visc, cor, depth, wetm, icem = held
    wet = wetm[...].astype(jnp.float32)
    active = wet * icem[...].astype(jnp.float32)
    visc = visc[...]
    depth = depth[...]
    mass = mass[...]
    cor = cor[...]
    gu, gv, gs = guess[0], guess[1], oguess[...]
    ai = active * visc
    ao = wet * depth
    full_i = active * (mass + 4.0 * visc * visc) + 1.0 - active
    full_o = wet * (1.0 + 4.0 * depth * depth) + 1.0 - wet
    pi = 1.0 / full_i
    po = 1.0 / full_o
    inv_ref[0] = pi
    inv_ref[1] = po
    ac = active * cor
    fields = [
        ai * gu,
        ai * gv,
        ao * gs,
        rhs[0] - (full_i * gu - ac * gv),
        rhs[1] - (full_i * gv + ac * gu),
        orhs[...] - full_o * gs,
        ai,
        ao,
        ai * pi,
        ao * po,
        ac * pi,
    ]
    for k, field in enumerate(fields):
        ext[k, 0:rows, 0:cols] = field

    send_e[...] = jnp.zeros_like(send_e)
    send_w[...] = jnp.zeros_like(send_w)
    for k, (width, place) in enumerate(zip(WIDTHS, PLACES)):
        send_w[place : place + width, :] = ext[k, 0:width, 0:cols]
        start = ROWS - place - width
        send_e[start : start + width, :] = ext[k, rows - width : rows, 0:cols]
    lane = lax.broadcasted_iota(jnp.int32, (rows, LANES), 1)
    low = jnp.zeros((rows, LANES), jnp.float32)
    high = jnp.zeros((rows, LANES), jnp.float32)
    for k, (width, place) in enumerate(zip(WIDTHS, PLACES)):
        first = ext[k, 0:rows, 0:LANES]
        last = ext[k, 0:rows, cols - LANES : cols]
        low = jnp.where((lane >= place) & (lane < place + width), rolled(first, place, 1), low)
        start = LANES - place - width
        high = jnp.where((lane >= start) & (lane < start + width), rolled(last, -place, 1), high)
    send_s[...] = low

    @pl.when(jnp.logical_not(top))
    def _():
        send_n[...] = high

    def negated(place):
        return (place < 6) | ((place >= 9) & (place < 13))

    @pl.when(top)
    def _():
        sign = jnp.where(negated(lane), -1.0, 1.0)
        send_n[...] = sign * flipped_lanes(flipped_rows(high))

    if flat:
        pl.semaphore_wait(barrier, total - 1)
    else:
        diagonals = 2 * (jnp.where(top, 0, 1) + jnp.where(bottom, 0, 1))
        pl.semaphore_wait(barrier, gx - 1 + gy - 1 + diagonals)

    def copy(source, where, slot, px, py):
        return pltpu.make_async_remote_copy(
            src_ref=source,
            dst_ref=where,
            send_sem=send_sem.at[slot],
            recv_sem=recv_sem.at[slot],
            device_id=(px, py),
            device_id_type=MESH,
        )

    mirror = gx - 1 - x
    fold_e = lax.rem(mirror + gx - 1, gx)
    fold_w = lax.rem(mirror + 1, gx)
    corner = [recv_corner.at[k] for k in range(4)]
    to_e = copy(send_e, recv_w.at[pl.ds(8, ROWS)], WEST, east, y)
    to_w = copy(send_w, recv_e.at[pl.ds(0, ROWS)], EAST, west, y)
    n_first, n_last = send_n.at[pl.ds(0, 8)], send_n.at[pl.ds(rows - 8, 8)]
    s_first, s_last = send_s.at[pl.ds(0, 8)], send_s.at[pl.ds(rows - 8, 8)]
    plain_n = [
        copy(send_n, recv_s, SOUTH, x, y + 1),
        copy(n_last, corner[SW - NE], SW, east, y + 1),
        copy(n_first, corner[SE - NE], SE, west, y + 1),
    ]
    fold_n = copy(send_n, recv_n, NORTH, mirror, y)
    fold_ne = copy(n_first, corner[NE - NE], NE, fold_e, y)
    fold_nw = copy(n_last, corner[NW - NE], NW, fold_w, y)
    plain_s = [
        copy(send_s, recv_n, NORTH, x, y - 1),
        copy(s_last, corner[NW - NE], NW, east, y - 1),
        copy(s_first, corner[NE - NE], NE, west, y - 1),
    ]
    away_e = top & (fold_e != x)
    away_w = top & (fold_w != x)

    to_e.start()
    to_w.start()

    @pl.when(top)
    def _():
        fold_n.start()

    @pl.when(away_e)
    def _():
        fold_ne.start()

    @pl.when(away_w)
    def _():
        fold_nw.start()

    @pl.when(top & (fold_e == x))
    def _():
        recv_corner[NE - NE] = send_n[0:8]

    @pl.when(top & (fold_w == x))
    def _():
        recv_corner[NW - NE] = send_n[rows - 8 : rows]

    @pl.when(jnp.logical_not(top))
    def _():
        for c in plain_n:
            c.start()

    @pl.when(jnp.logical_not(bottom))
    def _():
        for c in plain_s:
            c.start()

    @pl.when(jnp.logical_not(bottom))
    def _():
        for c in plain_n:
            c.wait_recv()

    plain_s[0].wait_recv()

    @pl.when(jnp.logical_not(top & (fold_e == x)))
    def _():
        plain_s[2].wait_recv()

    @pl.when(jnp.logical_not(top & (fold_w == x)))
    def _():
        plain_s[1].wait_recv()

    to_e.wait_recv()
    to_w.wait_recv()

    half = lax.broadcasted_iota(jnp.int32, (8, LANES), 0) < 4
    corner_n = jnp.where(half, recv_corner[NE - NE], recv_corner[NW - NE])
    corner_s = jnp.where(half, recv_corner[SE - NE], recv_corner[SW - NE])
    from_n = jnp.concatenate([recv_n[...], corner_n], axis=0)
    from_s = jnp.concatenate([recv_s[...], corner_s], axis=0)
    near = lax.broadcasted_iota(jnp.int32, (rows + 8, LANES), 1) < LANES // 2
    upper = lax.broadcasted_iota(jnp.int32, (8, cols), 0) < 4
    for k, place in enumerate(PLACES):
        ext[k, :, cols : cols + LANES] = jnp.where(
            near, rolled(from_n, -place, 1), rolled(from_s, place, 1)
        )
        end = 8 + ROWS - place
        ext[k, rows : rows + 8, 0:cols] = jnp.where(
            upper, recv_e[place : place + 8, :], recv_w[end - 8 : end, :]
        )

    ai, ao, si, so, c = (ext[k] for k in range(6, 11))
    ru = ext[3] + ai * beside(ext[0])
    rv = ext[4] + ai * beside(ext[1])
    rs = ext[5] + ao * beside(ext[2])
    nu = ai * beside(si * ru) + c * rv
    nv = ai * beside(si * rv) - c * ru
    ns = ao * beside(so * rs)
    mu = ai * beside(si * nu) + c * nv
    mv = ai * beside(si * nv) - c * nu
    ms = ao * beside(so * ns)

    def own(value):
        return value[0:rows, 0:cols]

    ru, rv, rs, nu, nv, ns, mu, mv, ms = map(own, (ru, rv, rs, nu, nv, ns, mu, mv, ms))
    pi, po = inv_ref[0], inv_ref[1]
    e1u, e1v, e1s = ru - nu, rv - nv, rs - ns
    e2u, e2v, e2s = nu - mu, nv - mv, ns - ms
    prs, pns = po * rs, po * ns
    products = [
        e1u * e1u + e1v * e1v,
        e1u * e2u + e1v * e2v,
        e2u * e2u + e2v * e2v,
        e1u * ru + e1v * rv,
        e2u * ru + e2v * rv,
        prs * e1s,
        pns * e1s,
        pns * e2s,
        pns * rs,
    ]
    spot = lax.broadcasted_iota(jnp.int32, (1, LANES), 1)
    spots = lax.broadcasted_iota(jnp.int32, (16, LANES), 0)
    tall = jnp.zeros((16, LANES), jnp.float32)
    for k, product in enumerate(products):
        halves = sum(product[:, p : p + LANES] for p in range(0, cols, LANES))
        tall = jnp.where(spots == k, jnp.sum(halves, axis=0, keepdims=True), tall)
    across = jnp.sum(tall, axis=1, keepdims=True)
    diagonal = spots == lax.broadcasted_iota(jnp.int32, (16, LANES), 1)
    packed = jnp.sum(jnp.where(diagonal, across, 0.0), axis=0, keepdims=True)

    def exchange(slot, count, mine, device, number, work=None):
        slot[mine] = packed_now[0]

        def one(k):
            return pltpu.make_async_remote_copy(
                src_ref=slot.at[mine],
                dst_ref=slot.at[mine],
                send_sem=sum_send.at[number],
                recv_sem=sum_recv.at[number],
                device_id=device(k),
                device_id_type=MESH,
            )

        @pl.loop(1, count)
        def _(k):
            one(k).start()

        if work is not None:
            work()
        most = slot.at[pl.ds(0, count - 1)]
        pltpu.make_async_copy(most, most, sum_recv.at[number]).wait()
        return jnp.sum(slot[...], axis=0)

    def scale():
        for k, value in enumerate((pi * ru, pi * rv, prs, pi * nu, pi * nv, pns)):
            scaled[k] = value

    packed_now = [packed]
    if flat:
        def anyone(k):
            other = lax.rem(me + k, total)
            return (other // gy, lax.rem(other, gy))

        packed = exchange(sums, total, me, anyone, 0, scale)
    else:
        packed_now[0] = exchange(
            sums.at[pl.ds(0, gx)], gx, x, lambda k: (lax.rem(x + k, gx), y), 0, scale
        )
        packed = exchange(
            sums.at[pl.ds(gx, gy)], gy, y, lambda k: (x, lax.rem(y + k, gy)), 1
        )
    s = [
        jnp.sum(jnp.where(spot == k, packed, 0.0), axis=1, keepdims=True) for k in range(SUMS)
    ]
    y1, y2 = two_by_two(s[0], s[1], s[2], s[3], s[4])
    d1, d2 = two_by_two(s[5], s[6], s[7], s[5] + s[8], s[8])
    out_ice[0] = held[1][0] + y1 * scaled[0] + y2 * scaled[3]
    out_ice[1] = held[1][1] + y1 * scaled[1] + y2 * scaled[4]
    out_ocean[...] = held[3][...] + d1 * scaled[2] + d2 * scaled[5]

    groups = [(sums, total)] if flat else [(sums.at[pl.ds(0, gx)], gx), (sums.at[pl.ds(gx, gy)], gy)]
    for number, (slot, count) in enumerate(groups):
        most = slot.at[pl.ds(0, count - 1)]
        pltpu.make_async_copy(most, most, sum_send.at[number]).wait()
    to_e.wait_send()
    to_w.wait_send()

    @pl.when(top)
    def _():
        fold_n.wait_send()

    @pl.when(away_e)
    def _():
        fold_ne.wait_send()

    @pl.when(away_w)
    def _():
        fold_nw.wait_send()

    @pl.when(jnp.logical_not(top))
    def _():
        for c in plain_n:
            c.wait_send()

    @pl.when(jnp.logical_not(bottom))
    def _():
        for c in plain_s:
            c.wait_send()


def store(ice, ocean, out_ice, out_ocean, sem):
    copies = [
        pltpu.make_async_copy(ice, out_ice, sem.at[0]),
        pltpu.make_async_copy(ocean, out_ocean, sem.at[1]),
    ]
    for c in copies:
        c.start()
    for c in copies:
        c.wait()


def solution(mesh):
    gx, gy = mesh.shape["gx"], mesh.shape["gy"]

    def body(*args):
        _, rows, cols = args[0].shape
        slots = gx * gy if gx * gy <= FLAT_LIMIT else gx + gy
        f32 = jnp.float32
        edge = pltpu.VMEM((rows, LANES), f32)
        strip = pltpu.VMEM((ROWS, cols), f32)
        tall = pltpu.VMEM((ROWS + 8, cols), f32)
        ice, ocean = pl.pallas_call(
            functools.partial(kernel, (gx, gy, rows, cols)),
            out_shape=(pltpu.VMEM((2, rows, cols), f32), pltpu.VMEM((rows, cols), f32)),
            in_specs=[pl.BlockSpec(memory_space=pl.ANY)] * 10,
            out_specs=(pl.BlockSpec(memory_space=pltpu.VMEM),) * 2,
            scratch_shapes=[pltpu.VMEM(a.shape, a.dtype) for a in args]
            + [
                pltpu.VMEM((len(WIDTHS), rows + 8, cols + LANES), f32),
                pltpu.VMEM((2, rows, cols), f32),
                strip, strip, edge, edge,
                tall, tall, edge, edge, pltpu.VMEM((4, 8, LANES), f32),
                pltpu.VMEM((6, rows, cols), f32),
                pltpu.VMEM((slots, 1, LANES), f32),
                pltpu.SemaphoreType.DMA((10,)),
                pltpu.SemaphoreType.DMA((8,)),
                pltpu.SemaphoreType.DMA((8,)),
                pltpu.SemaphoreType.DMA((2,)),
                pltpu.SemaphoreType.DMA((2,)),
            ],
            compiler_params=pltpu.CompilerParams(collective_id=0, has_side_effects=True),
            name="picard",
        )(*args)
        return pl.pallas_call(
            store,
            out_shape=(
                jax.ShapeDtypeStruct(ice.shape, f32),
                jax.ShapeDtypeStruct(ocean.shape, f32),
            ),
            in_specs=[pl.BlockSpec(memory_space=pltpu.VMEM)] * 2,
            out_specs=(pl.BlockSpec(memory_space=pl.ANY),) * 2,
            scratch_shapes=[pltpu.SemaphoreType.DMA((2,))],
            name="store",
        )(
            pltpu.with_memory_space_constraint(ice, pltpu.VMEM),
            pltpu.with_memory_space_constraint(ocean, pltpu.VMEM),
        )

    grid3, grid2 = P(None, "gx", "gy"), P("gx", "gy")
    return jax.shard_map(
        body,
        mesh=mesh,
        in_specs=(grid3, grid3) + (grid2,) * 8,
        out_specs=(grid3, grid2),
        check_vma=False,
    )
```
